32 devices in a mesh: span: 8 (over y, x, core), head: 4 (over z).
Axes of the slice: x: 2, y: 2, z: 4, core: 2. Of those that a mesh axis runs over, the one named last changes fastest.
Arguments:
- decoder_states: bfloat16 [16384, 1024], P('span'), may hold values from -21 to 21
- encodings: bfloat16 [512, 128, 1024], P('span', 'head'), may hold values from -21 to 21
- neighbor_table: int32 [256, 2, 2], P('span'), may hold values from 0 to 63, as said below
- query_weight: bfloat16 [1024, 1024], P(None, 'head'), may hold values from -0.1875 to 0.1875
- key_weight: bfloat16 [1024, 1024], P(None, 'head'), may hold values from -0.1875 to 0.1875
- value_weight: bfloat16 [1024, 1024], P(None, 'head'), may hold values from -0.1875 to 0.1875
- out_weight: bfloat16 [1024, 1024], P('head'), may hold values from -0.1875 to 0.1875
Outputs:
- attended: bfloat16 [16384, 1024], P('span', 'head')
The draws below stay inside these ranges and needn't reach their ends.
Inputs may be any that keep to these rules, and one draw needn't show every extreme that they name: neighbor_table[c, k, 0] is the database shard and neighbor_table[c, k, 1] the slot in that shard of neighbor k of span c; in each aligned block of 32 spans (the spans of one device along `span`) every shard is named by exactly one neighbor, and every slot of every shard is named exactly once in the whole table.
All inputs are finite; a program needn't handle non-finite values.
Results may differ from the reference program's by a relative error of at most 0.012.
The reference program's roundings to bfloat16 on the way (of `keys`, `values`, `queries`, `weights` and `context`) count: a program that leaves them out, or rounds other values in their place, can miss the bound.
Values may be sent and summed in bfloat16 or wider, within the bound.
A program may use at most 128 MiB of HBM per device.

```python
import jax
import jax.numpy as jnp
from jax import lax

D = 1024
HEADS = 16
HEAD_DIM = 64
SPAN_LEN = 64
NEIGH = 2
NTOK = 128
SEQ_LEN = 2048
SPANS_SEQ = 32
TOKENS = 16384
SPANS = 256
SHARDS = 8
SLOTS = 64
PER_SOURCE = 8


def draw_decoder_states(key, part):
    subkeys = jax.random.split(jax.random.fold_in(key, 3), 1)
    values = jnp.clip(jax.random.normal(subkeys[0], (TOKENS, D), jnp.float32), -6.0, 6.0)
    return values.astype(jnp.bfloat16)


def draw_encodings(key, part):
    subkeys = jax.random.split(jax.random.fold_in(key, 5), 1)
    shape_all = (SHARDS * SLOTS, NTOK, D)
    values = jnp.clip(jax.random.normal(subkeys[0], shape_all, jnp.float32), -6.0, 6.0)
    return values.astype(jnp.bfloat16)


def draw_neighbor_table(key, part):
    dest_keys = jax.random.split(jax.random.fold_in(key, 11), SHARDS)
    orders = jax.vmap(lambda subkey: jax.random.permutation(subkey, SLOTS))(dest_keys).astype(jnp.int32)
    shard_of = orders // PER_SOURCE
    sub_index = orders % PER_SOURCE
    source_keys = jax.random.split(jax.random.fold_in(key, 12), SHARDS)
    slot_orders = jax.vmap(lambda subkey: jax.random.permutation(subkey, SLOTS))(source_keys).astype(jnp.int32)
    destination = jnp.arange(SHARDS, dtype=jnp.int32)[:, None]
    slot_of = slot_orders[shard_of, destination * PER_SOURCE + sub_index]
    return jnp.stack([shard_of, slot_of], axis=-1).reshape(SPANS, NEIGH, 2).astype(jnp.int32)


def steps_of(rng, dims, pieces, smallest, largest):
    def one(position, parts):
        draws = jax.random.uniform(jax.random.fold_in(jax.random.fold_in(rng, 6), position), (parts,), jnp.float32, smallest / len(pieces), largest / len(pieces))
        return jnp.repeat(jnp.exp(draws), dims[position] // parts).reshape((-1,) + (1,) * (len(dims) - position - 1))

    level = one(*pieces[0])
    for cut in pieces[1:]:
        level = level * one(*cut)
    return level


def normal_values(key, dims, spread, bound, pieces=(), kind=jnp.bfloat16):
    drawn = jax.random.normal(key, dims, jnp.float32) * spread
    if len(pieces) > 0:
        drawn = steps_of(key, dims, pieces, -0.22, 0.18) * drawn
    return jnp.clip(drawn, min=-bound, max=bound).astype(kind)


def setup_inputs(seed: int = 0) -> dict:
    keys = jax.random.split(jax.random.key(seed), 8)
    decoder_states = draw_decoder_states(jax.random.fold_in(keys[7], 71), 0)
    encodings = draw_encodings(jax.random.fold_in(keys[7], 71), 0)
    neighbor_table = draw_neighbor_table(jax.random.fold_in(keys[7], 71), 0)
    query_weight = normal_values(keys[3], (D, HEADS * HEAD_DIM), D ** -0.5, 0.1875, ((1, 4),))
    key_weight = normal_values(keys[4], (D, HEADS * HEAD_DIM), D ** -0.5, 0.1875, ((1, 4),))
    value_weight = normal_values(keys[5], (D, HEADS * HEAD_DIM), D ** -0.5, 0.1875, ((1, 4),))
    out_weight = normal_values(keys[6], (HEADS * HEAD_DIM, D), (HEADS * HEAD_DIM) ** -0.5, 0.1875, ((0, 4),))
    return dict(decoder_states=decoder_states, encodings=encodings, neighbor_table=neighbor_table, query_weight=query_weight, key_weight=key_weight, value_weight=value_weight, out_weight=out_weight)


def reference(decoder_states, encodings, neighbor_table, query_weight, key_weight, value_weight, out_weight):
    group_rows = (neighbor_table[:, :, 0] * SLOTS + neighbor_table[:, :, 1]).astype(jnp.int32)
    inv_root = HEAD_DIM ** -0.5
    offset = SPAN_LEN - 1
    inner_width = HEADS * HEAD_DIM

    def one_sequence(sequence):
        states = lax.dynamic_slice_in_dim(decoder_states, sequence * SEQ_LEN, SEQ_LEN, 0)
        chosen = lax.dynamic_slice_in_dim(group_rows, sequence * SPANS_SEQ, SPANS_SEQ, 0).reshape(-1)
        flattened = encodings[chosen].reshape(-1, D)
        key_rows = jnp.dot(flattened, key_weight, preferred_element_type=jnp.float32).astype(jnp.bfloat16)
        key_rows = key_rows.reshape(SPANS_SEQ, NEIGH * NTOK, HEADS, HEAD_DIM)
        value_rows = jnp.dot(flattened, value_weight, preferred_element_type=jnp.float32).astype(jnp.bfloat16)
        value_rows = value_rows.reshape(SPANS_SEQ, NEIGH * NTOK, HEADS, HEAD_DIM)
        queries = jnp.dot(states, query_weight, preferred_element_type=jnp.float32).astype(jnp.bfloat16)
        shifted = jnp.concatenate([queries[offset:], jnp.zeros((offset, inner_width), jnp.bfloat16)], axis=0)
        shifted = shifted.reshape(SPANS_SEQ, SPAN_LEN, HEADS, HEAD_DIM)
        scores = jnp.einsum("cqhd,ckhd->chqk", shifted.astype(jnp.float32), key_rows.astype(jnp.float32)) * inv_root
        weights = jax.nn.softmax(scores, axis=-1).astype(jnp.bfloat16)
        context = jnp.einsum("chqk,ckhd->cqhd", weights.astype(jnp.float32), value_rows.astype(jnp.float32))
        context = context.astype(jnp.bfloat16).reshape(SEQ_LEN, inner_width)
        context = jnp.concatenate([jnp.zeros((offset, inner_width), jnp.bfloat16), context[:SEQ_LEN - offset]], axis=0)
        return jnp.dot(context, out_weight, preferred_element_type=jnp.float32).astype(jnp.bfloat16)

    sequences = TOKENS // SEQ_LEN
    outputs = lax.map(one_sequence, jnp.arange(sequences, dtype=jnp.int32))
    return outputs.reshape(TOKENS, D)
```

```python
import functools

import jax
import jax.numpy as jnp
from jax import lax
from jax.experimental import pallas as pl
from jax.experimental.pallas import tpu as pltpu
from jax.sharding import PartitionSpec as P

HEAD_DIM = 64
SPAN_LEN = 64
SEQ_LEN = 2048
VMEM = 56 * 1024 * 1024


def matmul_kernel(x_ref, w_ref, o_ref):
    w = w_ref[...].reshape(x_ref.shape[1], o_ref.shape[1])
    o_ref[...] = jnp.dot(x_ref[...], w, preferred_element_type=jnp.float32).astype(o_ref.dtype)


def grouped_matmul(x, w, cols, col_block, tile):
    peers, groups, depth, _ = w.shape
    rows, width = x.shape
    return pl.pallas_call(
        matmul_kernel,
        out_shape=jax.ShapeDtypeStruct((rows, groups * cols), jnp.bfloat16),
        grid=(groups, rows // tile),
        in_specs=[
            pl.BlockSpec((tile, width), lambda g, i: (i, 0)),
            pl.BlockSpec((peers, 1, depth, cols), lambda g, i: (0, g, 0, col_block)),
        ],
        out_specs=pl.BlockSpec((tile, cols), lambda g, i: (i, g)),
        compiler_params=pltpu.CompilerParams(vmem_limit_bytes=VMEM),
        cost_estimate=pl.CostEstimate(
            flops=2 * rows * width * groups * cols, bytes_accessed=16 << 20, transcendentals=0
        ),
    )(x, w)


def attend_kernel(position_ref, q_ref, kv_ref, ctx_ref, lse_ref, *, spans, neighbors, group_cols):
    step = pl.program_id(0)
    width = q_ref.shape[1]
    heads = width // HEAD_DIM
    packed = group_cols // HEAD_DIM
    tokens = kv_ref.shape[1]
    keys = neighbors * tokens
    wide = packed * keys
    row_head = lax.broadcasted_iota(jnp.int32, (wide, group_cols), 0) // keys
    col_head = lax.broadcasted_iota(jnp.int32, (wide, group_cols), 1) // HEAD_DIM
    diagonal = row_head == col_head
    lane_head = lax.broadcasted_iota(jnp.int32, (SPAN_LEN, wide), 1) // keys
    lse_lane = lax.broadcasted_iota(jnp.int32, (SPAN_LEN, 128), 1)
    lse_rows = []
    for c in range(spans):
        span = step * spans + c
        rows = [kv_ref[position_ref[span * neighbors + k]] for k in range(neighbors)]
        kv = jnp.concatenate(rows, axis=0)
        lse_all = jnp.zeros((SPAN_LEN, 128), jnp.float32)
        for g in range(width // group_cols):
            base = g * 2 * group_cols
            q = q_ref[c * SPAN_LEN : (c + 1) * SPAN_LEN, g * group_cols : (g + 1) * group_cols]
            k = kv[:, base : base + group_cols]
            v = kv[:, base + group_cols : base + 2 * group_cols]
            k_wide = jnp.where(diagonal, jnp.concatenate([k] * packed, axis=0), 0)
            v_wide = jnp.where(diagonal, jnp.concatenate([v] * packed, axis=0), 0)
            s = lax.dot_general(
                q, k_wide, (((1,), (1,)), ((), ())), preferred_element_type=jnp.float32
            ) * (HEAD_DIM ** (-0.5))
            top = jnp.zeros_like(s)
            tops = []
            for n in range(packed):
                m = jnp.max(jnp.where(lane_head == n, s, -jnp.inf), axis=1, keepdims=True)
                tops.append(m)
                top = jnp.where(lane_head == n, m, top)
            e = jnp.exp(s - top)
            inv = jnp.zeros_like(s)
            for n in range(packed):
                l = jnp.sum(jnp.where(lane_head == n, e, 0.0), axis=1, keepdims=True)
                inv = jnp.where(lane_head == n, 1.0 / l, inv)
                lse_all = jnp.where(lse_lane == g * packed + n, tops[n] + jnp.log(l), lse_all)
            p = (e * inv).astype(jnp.bfloat16)
            out = jnp.dot(p, v_wide, preferred_element_type=jnp.float32)
            ctx_ref[c * SPAN_LEN : (c + 1) * SPAN_LEN, g * group_cols : (g + 1) * group_cols] = (
                out.astype(ctx_ref.dtype)
            )
        lse_rows.append(lse_all)
    lse_ref[...] = jnp.concatenate(lse_rows, axis=0).T[:heads]


def attend(position, q, kv, span_count, neighbors, group_cols, spans=2):
    rows, width = q.shape
    heads = width // HEAD_DIM
    entries, tokens, wide = kv.shape
    return pl.pallas_call(
        functools.partial(
            attend_kernel, spans=spans, neighbors=neighbors, group_cols=group_cols
        ),
        out_shape=(
            jax.ShapeDtypeStruct((rows, width), jnp.bfloat16),
            jax.ShapeDtypeStruct((heads, rows), jnp.float32),
        ),
        grid_spec=pltpu.PrefetchScalarGridSpec(
            num_scalar_prefetch=1,
            grid=(span_count // spans,),
            in_specs=[
                pl.BlockSpec((spans * SPAN_LEN, width), lambda i, p: (i, 0)),
                pl.BlockSpec((entries, tokens, wide), lambda i, p: (0, 0, 0)),
            ],
            out_specs=[
                pl.BlockSpec((spans * SPAN_LEN, width), lambda i, p: (i, 0)),
                pl.BlockSpec((heads, spans * SPAN_LEN), lambda i, p: (0, i)),
            ],
        ),
        compiler_params=pltpu.CompilerParams(vmem_limit_bytes=VMEM),
        cost_estimate=pl.CostEstimate(
            flops=2 << 32, bytes_accessed=16 << 20, transcendentals=1 << 21
        ),
    )(position, q, kv)


def project_kernel(ctx_ref, own_ref, all_ref, w_ref, o_ref):
    own = own_ref[...]
    every = all_ref[...]
    top = jnp.max(every, axis=0)
    total = jnp.sum(jnp.exp(every - top[None]), axis=0)
    scale = jnp.exp(own - top) / total
    high = scale.astype(jnp.bfloat16)
    low = (scale - high.astype(jnp.float32)).astype(jnp.bfloat16)
    heads = scale.shape[0]
    width = ctx_ref.shape[1]
    spread = (
        lax.broadcasted_iota(jnp.int32, (2 * heads, width), 0) % heads
        == lax.broadcasted_iota(jnp.int32, (2 * heads, width), 1) // HEAD_DIM
    ).astype(jnp.bfloat16)
    factor = lax.dot_general(
        jnp.concatenate([high, low], axis=0),
        spread,
        (((0,), (0,)), ((), ())),
        preferred_element_type=jnp.float32,
    )
    scaled = (ctx_ref[...].astype(jnp.float32) * factor).astype(jnp.bfloat16)
    o_ref[...] = jnp.dot(scaled, w_ref[...], preferred_element_type=jnp.float32).astype(
        o_ref.dtype
    )


def project(ctx, own, every, w, tile=512):
    rows, width = ctx.shape
    groups, heads, _ = every.shape
    return pl.pallas_call(
        project_kernel,
        out_shape=jax.ShapeDtypeStruct((rows, w.shape[1]), jnp.bfloat16),
        grid=(rows // tile,),
        in_specs=[
            pl.BlockSpec((tile, width), lambda i: (i, 0)),
            pl.BlockSpec((heads, tile), lambda i: (0, i)),
            pl.BlockSpec((groups, heads, tile), lambda i: (0, 0, i)),
            pl.BlockSpec(w.shape, lambda i: (0, 0)),
        ],
        out_specs=pl.BlockSpec((tile, w.shape[1]), lambda i: (i, 0)),
        compiler_params=pltpu.CompilerParams(vmem_limit_bytes=VMEM),
    )(ctx, own, every, w)


def body(
    decoder_states, encodings, neighbor_table, query_weight, key_weight, value_weight, out_weight
):
    peer_count = lax.axis_size("span")
    groups = lax.axis_size("head")
    model_width = decoder_states.shape[1]
    group_cols = query_weight.shape[1]
    me = lax.axis_index("span")
    packed = jnp.concatenate([key_weight, value_weight, query_weight], axis=1)
    part = model_width // peer_count
    packed = lax.dynamic_slice_in_dim(packed, me * part, part, 0)
    gathered = lax.all_gather(packed, ("span", "head"), axis=0, tiled=False)
    gathered = gathered.reshape(peer_count, groups, part, 3 * group_cols)
    out_part = group_cols // peer_count
    out_slice = lax.dynamic_slice_in_dim(out_weight, me * out_part, out_part, 0)
    out_all = lax.all_gather(out_slice, ("head", "span"), axis=0, tiled=True)

    shard_ids = neighbor_table[:, :, 0].reshape(-1)
    slot_ids = neighbor_table[:, :, 1].reshape(-1)
    entries = shard_ids.shape[0]
    per_peer = entries // peer_count
    numbering = jnp.arange(entries, dtype=jnp.int32)
    same_before = (shard_ids[:, None] == shard_ids[None, :]) & (
        numbering[None, :] < numbering[:, None]
    )
    ranking = jnp.sum(same_before.astype(jnp.int32), axis=1)
    position = shard_ids * per_peer + ranking
    placed = position[None, :] == numbering[:, None]
    request = jnp.sum(jnp.where(placed, slot_ids[None, :], 0), axis=1)
    wanted = lax.all_to_all(request, "span", split_axis=0, concat_axis=0, tiled=True)
    selected = encodings[wanted]
    arrived = lax.all_to_all(selected, "span", split_axis=0, concat_axis=0, tiled=True)

    sequences = decoder_states.shape[0] // SEQ_LEN
    offset = SPAN_LEN - 1
    states = decoder_states.reshape(sequences, SEQ_LEN, model_width)
    states = jnp.concatenate(
        [states[:, offset:], jnp.zeros((sequences, offset, model_width), states.dtype)], axis=1
    ).reshape(-1, model_width)
    tile = min(1024, decoder_states.shape[0])
    queries = grouped_matmul(states, gathered, group_cols, 2, tile)
    kv = grouped_matmul(arrived.reshape(-1, model_width), gathered, 2 * group_cols, 0, tile)
    kv = kv.reshape(entries, arrived.shape[1], -1)
    context, lse = attend(
        position, queries, kv, neighbor_table.shape[0], neighbor_table.shape[1], group_cols
    )
    every = lax.all_gather(lse, "head", axis=0, tiled=False)
    partial = project(context, lse, every, out_all)
    summed = lax.psum_scatter(partial, "head", scatter_dimension=1, tiled=True)
    summed = summed.reshape(sequences, SEQ_LEN, -1)
    summed = jnp.concatenate(
        [jnp.zeros((sequences, offset, summed.shape[2]), summed.dtype), summed[:, :-offset]], axis=1
    )
    return summed.reshape(decoder_states.shape[0], -1)


def solution(mesh):
    return jax.shard_map(
        body,
        mesh=mesh,
        in_specs=(
            P("span", None),
            P("span", "head", None),
            P("span", None, None),
            P(None, "head"),
            P(None, "head"),
            P(None, "head"),
            P("head", None),
        ),
        out_specs=P("span", "head"),
        check_vma=False,
    )
```

```python
import functools

import jax
import jax.numpy as jnp
from jax import lax
from jax.experimental import pallas as pl
from jax.experimental.pallas import tpu as pltpu
from jax.sharding import PartitionSpec as P

HEAD_DIM = 64
SPAN_LEN = 64
SEQ_LEN = 2048
VMEM = 56 * 1024 * 1024
CHUNKS = 2


def matmul_kernel(x_ref, w_ref, o_ref):
    groups = w_ref.shape[1]
    cols = w_ref.shape[3]
    x = x_ref[...]
    for g in range(groups):
        w = w_ref[:, g].reshape(x_ref.shape[1], cols)
        o_ref[:, g * cols : (g + 1) * cols] = jnp.dot(
            x, w, preferred_element_type=jnp.float32
        ).astype(o_ref.dtype)


def grouped_matmul(x, w, cols, col_block, tile):
    peers, groups, depth, _ = w.shape
    rows, width = x.shape
    return pl.pallas_call(
        matmul_kernel,
        out_shape=jax.ShapeDtypeStruct((rows, groups * cols), jnp.bfloat16),
        grid=(rows // tile,),
        in_specs=[
            pl.BlockSpec((tile, width), lambda i: (i, 0)),
            pl.BlockSpec((peers, groups, depth, cols), lambda i: (0, 0, 0, col_block)),
        ],
        out_specs=pl.BlockSpec((tile, groups * cols), lambda i: (i, 0)),
        compiler_params=pltpu.CompilerParams(vmem_limit_bytes=VMEM),
        cost_estimate=pl.CostEstimate(
            flops=2 * rows * width * groups * cols, bytes_accessed=16 << 20, transcendentals=0
        ),
    )(x, w)


def attend_kernel(position_ref, *refs, spans, neighbors, group_cols):
    kv_refs = refs[: spans * neighbors]
    q_ref, ctx_ref, lse_ref, top_ref, s_ref, e_ref = refs[spans * neighbors :]
    width = q_ref.shape[1]
    heads = width // HEAD_DIM
    groups = width // group_cols
    packed = group_cols // HEAD_DIM
    tokens = kv_refs[0].shape[1]
    keys = neighbors * tokens
    wide = packed * keys
    row_head = lax.broadcasted_iota(jnp.int32, (wide, group_cols), 0) // keys
    col_head = lax.broadcasted_iota(jnp.int32, (wide, group_cols), 1) // HEAD_DIM
    diagonal = row_head == col_head
    pair = 128 // keys
    lane_head = lax.broadcasted_iota(jnp.int32, (SPAN_LEN, 128), 1) // keys
    lane = lax.broadcasted_iota(jnp.int32, (SPAN_LEN, 128), 1)
    collect = (
        lax.broadcasted_iota(jnp.int32, (heads * keys, 128), 0) // keys
        == lax.broadcasted_iota(jnp.int32, (heads * keys, 128), 1)
    ).astype(jnp.bfloat16)

    def widened(c, base):
        part = jnp.concatenate(
            [kv_refs[c * neighbors + k][0, :, base : base + group_cols] for k in range(neighbors)],
            axis=0,
        )
        return jnp.where(diagonal, jnp.concatenate([part] * packed, axis=0), 0)

    for c in range(spans):
        row = slice(c * SPAN_LEN, (c + 1) * SPAN_LEN)
        for g in range(groups):
            s_ref[row, g * wide : (g + 1) * wide] = lax.dot_general(
                q_ref[row, g * group_cols : (g + 1) * group_cols],
                widened(c, g * 2 * group_cols),
                (((1,), (1,)), ((), ())),
                preferred_element_type=jnp.float32,
            ) * (HEAD_DIM ** (-0.5))
    tops = []
    for c in range(spans):
        row = slice(c * SPAN_LEN, (c + 1) * SPAN_LEN)
        top_all = jnp.zeros((SPAN_LEN, 128), jnp.float32)
        for t in range(heads // pair):
            s = s_ref[row, t * 128 : (t + 1) * 128]
            top = None
            for n in range(pair):
                m = jnp.max(
                    jnp.where(lane_head == n, s, -jnp.inf), axis=1, keepdims=True
                )
                top = m if top is None else jnp.where(lane_head == n, m, top)
                top_all = jnp.where(lane == t * pair + n, m, top_all)
            e_ref[row, t * 128 : (t + 1) * 128] = jnp.exp(s - top).astype(jnp.bfloat16)
        tops.append(top_all)
    top_all = jnp.concatenate(tops, axis=0)
    total = jnp.dot(e_ref[...], collect, preferred_element_type=jnp.float32)
    top_rows = top_all.T[:heads]
    top_ref[...] = top_rows
    lse_ref[...] = top_rows + jnp.log(total.T[:heads])
    for c in range(spans):
        row = slice(c * SPAN_LEN, (c + 1) * SPAN_LEN)
        for g in range(groups):
            ctx_ref[row, g * group_cols : (g + 1) * group_cols] = jnp.dot(
                e_ref[row, g * wide : (g + 1) * wide],
                widened(c, g * 2 * group_cols + group_cols),
                preferred_element_type=jnp.float32,
            ).astype(ctx_ref.dtype)


def attend(position, q, kv, first, span_count, neighbors, group_cols, spans=4):
    width = q.shape[1]
    rows = span_count * SPAN_LEN
    heads = width // HEAD_DIM
    _, tokens, wide = kv.shape
    score_cols = heads * neighbors * tokens
    begin = first // spans
    step_rows = spans * SPAN_LEN

    def neighbor_spec(j):
        return pl.BlockSpec(
            (1, tokens, wide),
            lambda i, p: (p[(i + begin) * (spans * neighbors) + j], 0, 0),
        )

    return pl.pallas_call(
        functools.partial(
            attend_kernel, spans=spans, neighbors=neighbors, group_cols=group_cols
        ),
        out_shape=(
            jax.ShapeDtypeStruct((rows, width), jnp.bfloat16),
            jax.ShapeDtypeStruct((heads, rows), jnp.float32),
            jax.ShapeDtypeStruct((heads, rows), jnp.float32),
        ),
        grid_spec=pltpu.PrefetchScalarGridSpec(
            num_scalar_prefetch=1,
            grid=(span_count // spans,),
            in_specs=[neighbor_spec(j) for j in range(spans * neighbors)]
            + [pl.BlockSpec((step_rows, width), lambda i, p: (i + begin, 0))],
            out_specs=[
                pl.BlockSpec((step_rows, width), lambda i, p: (i, 0)),
                pl.BlockSpec((heads, step_rows), lambda i, p: (0, i)),
                pl.BlockSpec((heads, step_rows), lambda i, p: (0, i)),
            ],
            scratch_shapes=[
                pltpu.VMEM((step_rows, score_cols), jnp.float32),
                pltpu.VMEM((step_rows, score_cols), jnp.bfloat16),
            ],
        ),
        compiler_params=pltpu.CompilerParams(vmem_limit_bytes=VMEM),
        cost_estimate=pl.CostEstimate(
            flops=span_count << 28, bytes_accessed=16 << 20, transcendentals=span_count << 16
        ),
    )(position, *([kv] * (spans * neighbors)), q)


def project_kernel(ctx_ref, own_ref, all_ref, w_ref, o_ref):
    every = all_ref[...]
    top = jnp.max(every, axis=0)
    total = jnp.sum(jnp.exp(every - top[None]), axis=0)
    scale = jnp.exp(own_ref[...] - top) / total
    high = scale.astype(jnp.bfloat16)
    low = (scale - high.astype(jnp.float32)).astype(jnp.bfloat16)
    heads = scale.shape[0]
    width = ctx_ref.shape[1]
    spread = (
        lax.broadcasted_iota(jnp.int32, (2 * heads, width), 0) % heads
        == lax.broadcasted_iota(jnp.int32, (2 * heads, width), 1) // HEAD_DIM
    ).astype(jnp.bfloat16)
    factor = lax.dot_general(
        jnp.concatenate([high, low], axis=0),
        spread,
        (((0,), (0,)), ((), ())),
        preferred_element_type=jnp.float32,
    )
    scaled = (ctx_ref[...].astype(jnp.float32) * factor).astype(jnp.bfloat16)
    o_ref[...] = jnp.dot(scaled, w_ref[...], preferred_element_type=jnp.float32).astype(
        o_ref.dtype
    )


def project(ctx, own, every, w, tile=256):
    rows, width = ctx.shape
    groups, heads, _ = every.shape
    return pl.pallas_call(
        project_kernel,
        out_shape=jax.ShapeDtypeStruct((rows, w.shape[1]), jnp.bfloat16),
        grid=(rows // tile,),
        in_specs=[
            pl.BlockSpec((tile, width), lambda i: (i, 0)),
            pl.BlockSpec((heads, tile), lambda i: (0, i)),
            pl.BlockSpec((groups, heads, tile), lambda i: (0, 0, i)),
            pl.BlockSpec(w.shape, lambda i: (0, 0)),
        ],
        out_specs=pl.BlockSpec((tile, w.shape[1]), lambda i: (i, 0)),
        compiler_params=pltpu.CompilerParams(vmem_limit_bytes=VMEM),
        cost_estimate=pl.CostEstimate(
            flops=2 * rows * width * w.shape[1], bytes_accessed=6 << 20, transcendentals=0
        ),
    )(ctx, own, every, w)


def body(
    decoder_states, encodings, neighbor_table, query_weight, key_weight, value_weight, out_weight
):
    peer_count = lax.axis_size("span")
    groups = lax.axis_size("head")
    model_width = decoder_states.shape[1]
    group_cols = query_weight.shape[1]
    me = lax.axis_index("span")
    packed = jnp.concatenate([key_weight, value_weight, query_weight], axis=1)
    part = model_width // peer_count
    packed = lax.dynamic_slice_in_dim(packed, me * part, part, 0)
    gathered = lax.all_gather(packed, ("span", "head"), axis=0, tiled=False)
    gathered = gathered.reshape(peer_count, groups, part, 3 * group_cols)
    out_part = group_cols // peer_count
    out_slice = lax.dynamic_slice_in_dim(out_weight, me * out_part, out_part, 0)
    out_all = lax.all_gather(out_slice, ("head", "span"), axis=0, tiled=True)

    shard_ids = neighbor_table[:, :, 0].reshape(-1)
    slot_ids = neighbor_table[:, :, 1].reshape(-1)
    entries = shard_ids.shape[0]
    per_peer = entries // peer_count
    numbering = jnp.arange(entries, dtype=jnp.int32)
    same_before = (shard_ids[:, None] == shard_ids[None, :]) & (
        numbering[None, :] < numbering[:, None]
    )
    ranking = jnp.sum(same_before.astype(jnp.int32), axis=1)
    position = shard_ids * per_peer + ranking
    placed = position[None, :] == numbering[:, None]
    request = jnp.sum(jnp.where(placed, slot_ids[None, :], 0), axis=1)
    wanted = lax.all_to_all(request, "span", split_axis=0, concat_axis=0, tiled=True)
    selected = encodings[wanted]
    arrived = lax.all_to_all(selected, "span", split_axis=0, concat_axis=0, tiled=True)

    sequences = decoder_states.shape[0] // SEQ_LEN
    offset = SPAN_LEN - 1
    states = decoder_states.reshape(sequences, SEQ_LEN, model_width)
    states = jnp.concatenate(
        [states[:, offset:], jnp.zeros((sequences, offset, model_width), states.dtype)], axis=1
    ).reshape(-1, model_width)
    tile = 512
    queries = grouped_matmul(states, gathered, group_cols, 2, tile)
    kv = grouped_matmul(arrived.reshape(-1, model_width), gathered, 2 * group_cols, 0, tile)
    kv = kv.reshape(entries, arrived.shape[1], -1)
    span_count, neighbors = neighbor_table.shape[:2]
    pieces = []
    chunk = span_count // CHUNKS
    for first in range(0, span_count, chunk):
        context, lse, top = attend(position, queries, kv, first, chunk, neighbors, group_cols)
        every = lax.all_gather(lse, "head", axis=0, tiled=False)
        partial = project(context, top, every, out_all)
        pieces.append(lax.psum_scatter(partial, "head", scatter_dimension=1, tiled=True))
    summed = jnp.concatenate(pieces, axis=0)
    summed = summed.reshape(sequences, SEQ_LEN, -1)
    summed = jnp.concatenate(
        [jnp.zeros((sequences, offset, summed.shape[2]), summed.dtype), summed[:, :-offset]], axis=1
    )
    return summed.reshape(decoder_states.shape[0], -1)


def solution(mesh):
    return jax.shard_map(
        body,
        mesh=mesh,
        in_specs=(
            P("span", None),
            P("span", "head", None),
            P("span", None, None),
            P(None, "head"),
            P(None, "head"),
            P(None, "head"),
            P("head", None),
        ),
        out_specs=P("span", "head"),
        check_vma=False,
    )
```

```python
import functools

import jax
import jax.numpy as jnp
from jax import lax
from jax.experimental import pallas as pl
from jax.experimental.pallas import tpu as pltpu
from jax.sharding import PartitionSpec as P

HEAD_DIM = 64
SPAN_LEN = 64
SEQ_LEN = 2048
VMEM = 56 * 1024 * 1024
CHUNKS = 2


def matmul_kernel(x_ref, w_ref, o_ref):
    groups = w_ref.shape[1]
    cols = w_ref.shape[3]
    x = x_ref[...]
    for g in range(groups):
        w = w_ref[:, g].reshape(x_ref.shape[1], cols)
        o_ref[:, g * cols : (g + 1) * cols] = jnp.dot(
            x, w, preferred_element_type=jnp.float32
        ).astype(o_ref.dtype)


def grouped_matmul(x, w, cols, col_block, tile):
    peers, groups, depth, _ = w.shape
    rows, width = x.shape
    return pl.pallas_call(
        matmul_kernel,
        out_shape=jax.ShapeDtypeStruct((rows, groups * cols), jnp.bfloat16),
        grid=(rows // tile,),
        in_specs=[
            pl.BlockSpec((tile, width), lambda i: (i, 0)),
            pl.BlockSpec((peers, groups, depth, cols), lambda i: (0, 0, 0, col_block)),
        ],
        out_specs=pl.BlockSpec((tile, groups * cols), lambda i: (i, 0)),
        compiler_params=pltpu.CompilerParams(vmem_limit_bytes=VMEM),
        cost_estimate=pl.CostEstimate(
            flops=2 * rows * width * groups * cols, bytes_accessed=16 << 20, transcendentals=0
        ),
    )(x, w)


def attend_kernel(position_ref, *refs, spans, neighbors, group_cols):
    kv_refs = refs[: spans * neighbors]
    q_ref, ctx_ref, lse_ref, top_ref, s_ref, e_ref = refs[spans * neighbors :]
    width = q_ref.shape[1]
    heads = width // HEAD_DIM
    groups = width // group_cols
    packed = group_cols // HEAD_DIM
    tokens = kv_refs[0].shape[1]
    keys = neighbors * tokens
    wide = packed * keys
    row_head = lax.broadcasted_iota(jnp.int32, (wide, group_cols), 0) // keys
    col_head = lax.broadcasted_iota(jnp.int32, (wide, group_cols), 1) // HEAD_DIM
    diagonal = row_head == col_head
    pair = 128 // keys
    lane_head = lax.broadcasted_iota(jnp.int32, (SPAN_LEN, 128), 1) // keys
    lane = lax.broadcasted_iota(jnp.int32, (SPAN_LEN, 128), 1)
    collect = (
        lax.broadcasted_iota(jnp.int32, (heads * keys, 128), 0) // keys
        == lax.broadcasted_iota(jnp.int32, (heads * keys, 128), 1)
    ).astype(jnp.bfloat16)

    def widened(c, base):
        part = jnp.concatenate(
            [kv_refs[c * neighbors + k][0, :, base : base + group_cols] for k in range(neighbors)],
            axis=0,
        )
        return jnp.where(diagonal, jnp.concatenate([part] * packed, axis=0), 0)

    for c in range(spans):
        row = slice(c * SPAN_LEN, (c + 1) * SPAN_LEN)
        for g in range(groups):
            s_ref[row, g * wide : (g + 1) * wide] = lax.dot_general(
                q_ref[row, g * group_cols : (g + 1) * group_cols],
                widened(c, g * 2 * group_cols),
                (((1,), (1,)), ((), ())),
                preferred_element_type=jnp.float32,
            ) * (HEAD_DIM ** (-0.5))
    tops = []
    for c in range(spans):
        row = slice(c * SPAN_LEN, (c + 1) * SPAN_LEN)
        top_all = jnp.zeros((SPAN_LEN, 128), jnp.float32)
        for t in range(heads // pair):
            s = s_ref[row, t * 128 : (t + 1) * 128]
            top = None
            for n in range(pair):
                m = jnp.max(
                    jnp.where(lane_head == n, s, -jnp.inf), axis=1, keepdims=True
                )
                top = m if top is None else jnp.where(lane_head == n, m, top)
                top_all = jnp.where(lane == t * pair + n, m, top_all)
            e_ref[row, t * 128 : (t + 1) * 128] = jnp.exp(s - top).astype(jnp.bfloat16)
        tops.append(top_all)
    top_all = jnp.concatenate(tops, axis=0)
    total = jnp.dot(e_ref[...], collect, preferred_element_type=jnp.float32)
    top_rows = top_all.T[:heads]
    top_ref[...] = top_rows
    lse_ref[...] = top_rows + jnp.log(total.T[:heads])
    for c in range(spans):
        row = slice(c * SPAN_LEN, (c + 1) * SPAN_LEN)
        for g in range(groups):
            ctx_ref[row, g * group_cols : (g + 1) * group_cols] = jnp.dot(
                e_ref[row, g * wide : (g + 1) * wide],
                widened(c, g * 2 * group_cols + group_cols),
                preferred_element_type=jnp.float32,
            ).astype(ctx_ref.dtype)


def attend(position, q, kv, first, span_count, neighbors, group_cols, spans=4):
    width = q.shape[1]
    rows = span_count * SPAN_LEN
    heads = width // HEAD_DIM
    _, tokens, wide = kv.shape
    score_cols = heads * neighbors * tokens
    begin = first // spans
    step_rows = spans * SPAN_LEN

    def neighbor_spec(j):
        return pl.BlockSpec(
            (1, tokens, wide),
            lambda i, p: (p[(i + begin) * (spans * neighbors) + j], 0, 0),
        )

    return pl.pallas_call(
        functools.partial(
            attend_kernel, spans=spans, neighbors=neighbors, group_cols=group_cols
        ),
        out_shape=(
            jax.ShapeDtypeStruct((rows, width), jnp.bfloat16),
            jax.ShapeDtypeStruct((heads, rows), jnp.float32),
            jax.ShapeDtypeStruct((heads, rows), jnp.float32),
        ),
        grid_spec=pltpu.PrefetchScalarGridSpec(
            num_scalar_prefetch=1,
            grid=(span_count // spans,),
            in_specs=[neighbor_spec(j) for j in range(spans * neighbors)]
            + [pl.BlockSpec((step_rows, width), lambda i, p: (i + begin, 0))],
            out_specs=[
                pl.BlockSpec((step_rows, width), lambda i, p: (i, 0)),
                pl.BlockSpec((heads, step_rows), lambda i, p: (0, i)),
                pl.BlockSpec((heads, step_rows), lambda i, p: (0, i)),
            ],
            scratch_shapes=[
                pltpu.VMEM((step_rows, score_cols), jnp.float32),
                pltpu.VMEM((step_rows, score_cols), jnp.bfloat16),
            ],
        ),
        compiler_params=pltpu.CompilerParams(vmem_limit_bytes=VMEM),
        cost_estimate=pl.CostEstimate(
            flops=span_count << 28, bytes_accessed=16 << 20, transcendentals=span_count << 16
        ),
    )(position, *([kv] * (spans * neighbors)), q)


def project_kernel(ctx_ref, own_ref, all_ref, w_ref, o_ref):
    every = all_ref[...]
    top = jnp.max(every, axis=0)
    total = jnp.sum(jnp.exp(every - top[None]), axis=0)
    scale = jnp.exp(own_ref[...] - top) / total
    high = scale.astype(jnp.bfloat16)
    low = (scale - high.astype(jnp.float32)).astype(jnp.bfloat16)
    heads = scale.shape[0]
    width = ctx_ref.shape[1]
    spread = (
        lax.broadcasted_iota(jnp.int32, (2 * heads, width), 0) % heads
        == lax.broadcasted_iota(jnp.int32, (2 * heads, width), 1) // HEAD_DIM
    ).astype(jnp.bfloat16)
    factor = lax.dot_general(
        jnp.concatenate([high, low], axis=0),
        spread,
        (((0,), (0,)), ((), ())),
        preferred_element_type=jnp.float32,
    )
    scaled = (ctx_ref[...].astype(jnp.float32) * factor).astype(jnp.bfloat16)
    o_ref[...] = jnp.dot(scaled, w_ref[...], preferred_element_type=jnp.float32).astype(
        o_ref.dtype
    )


def project(ctx, own, every, w, tile=256):
    rows, width = ctx.shape
    groups, heads, _ = every.shape
    return pl.pallas_call(
        project_kernel,
        out_shape=jax.ShapeDtypeStruct((rows, w.shape[1]), jnp.bfloat16),
        grid=(rows // tile,),
        in_specs=[
            pl.BlockSpec((tile, width), lambda i: (i, 0)),
            pl.BlockSpec((heads, tile), lambda i: (0, i)),
            pl.BlockSpec((groups, heads, tile), lambda i: (0, 0, i)),
            pl.BlockSpec(w.shape, lambda i: (0, 0)),
        ],
        out_specs=pl.BlockSpec((tile, w.shape[1]), lambda i: (i, 0)),
        compiler_params=pltpu.CompilerParams(vmem_limit_bytes=VMEM),
        cost_estimate=pl.CostEstimate(
            flops=2 * rows * width * w.shape[1], bytes_accessed=6 << 20, transcendentals=0
        ),
    )(ctx, own, every, w)


def body(
    decoder_states, encodings, neighbor_table, query_weight, key_weight, value_weight, out_weight
):
    peer_count = lax.axis_size("span")
    groups = lax.axis_size("head")
    model_width = decoder_states.shape[1]
    group_cols = query_weight.shape[1]
    me = lax.axis_index("span")
    packed = jnp.concatenate([key_weight, value_weight, query_weight], axis=1)
    part = model_width // peer_count
    packed = lax.dynamic_slice_in_dim(packed, me * part, part, 0)
    gathered = lax.all_gather(packed, ("span", "head"), axis=0, tiled=False)
    gathered = gathered.reshape(peer_count, groups, part, 3 * group_cols)
    shard_ids = neighbor_table[:, :, 0].reshape(-1)
    slot_ids = neighbor_table[:, :, 1].reshape(-1)
    entries = shard_ids.shape[0]
    per_peer = entries // peer_count
    numbering = jnp.arange(entries, dtype=jnp.int32)
    same_before = (shard_ids[:, None] == shard_ids[None, :]) & (
        numbering[None, :] < numbering[:, None]
    )
    ranking = jnp.sum(same_before.astype(jnp.int32), axis=1)
    position = shard_ids * per_peer + ranking
    placed = position[None, :] == numbering[:, None]
    request = jnp.sum(jnp.where(placed, slot_ids[None, :], 0), axis=1)
    wanted = lax.all_to_all(request, "span", split_axis=0, concat_axis=0, tiled=True)
    wanted, late_out = lax.optimization_barrier((wanted, out_weight))
    out_all = lax.all_gather(late_out, "head", axis=0, tiled=True)
    selected = encodings[wanted]
    arrived = lax.all_to_all(selected, "span", split_axis=0, concat_axis=0, tiled=True)

    sequences = decoder_states.shape[0] // SEQ_LEN
    offset = SPAN_LEN - 1
    states = decoder_states.reshape(sequences, SEQ_LEN, model_width)
    states = jnp.concatenate(
        [states[:, offset:], jnp.zeros((sequences, offset, model_width), states.dtype)], axis=1
    ).reshape(-1, model_width)
    tile = 512
    queries = grouped_matmul(states, gathered, group_cols, 2, tile)
    kv = grouped_matmul(arrived.reshape(-1, model_width), gathered, 2 * group_cols, 0, tile)
    kv = kv.reshape(entries, arrived.shape[1], -1)
    span_count, neighbors = neighbor_table.shape[:2]
    pieces = []
    chunk = span_count // CHUNKS
    for first in range(0, span_count, chunk):
        context, lse, top = attend(position, queries, kv, first, chunk, neighbors, group_cols)
        every = lax.all_gather(lse, "head", axis=0, tiled=False)
        partial = project(context, top, every, out_all)
        pieces.append(lax.psum_scatter(partial, "head", scatter_dimension=1, tiled=True))
    summed = jnp.concatenate(pieces, axis=0)
    summed = summed.reshape(sequences, SEQ_LEN, -1)
    summed = jnp.concatenate(
        [jnp.zeros((sequences, offset, summed.shape[2]), summed.dtype), summed[:, :-offset]], axis=1
    )
    return summed.reshape(decoder_states.shape[0], -1)


def solution(mesh):
    return jax.shard_map(
        body,
        mesh=mesh,
        in_specs=(
            P("span", None),
            P("span", "head", None),
            P("span", None, None),
            P(None, "head"),
            P(None, "head"),
            P(None, "head"),
            P("head", None),
        ),
        out_specs=P("span", "head"),
        check_vma=False,
    )
```
